32 devices in a mesh: pulse: 16 (over z, y, core), rng: 2 (over x).
Axes of the slice: x: 2, y: 2, z: 4, core: 2. Of those that a mesh axis runs over, the one named last changes fastest.
Arguments:
- raw_pulses: bfloat16 [2, 512, 8192], P(None, 'pulse', 'rng'), may hold values from -6 to 6
- azimuth_taps: float32 [2, 9], replicated, may hold values from -1.5 to 1.5
- range_taps: bfloat16 [2, 128], replicated, may hold values from -0.375 to 0.375
- steering: bfloat16 [2, 32, 32], replicated, may hold values from -0.75 to 0.75
- angle_mats: bfloat16 [4, 2, 32, 32], replicated, may hold values from -0.75 to 0.75
- range_resampler_matrices: bfloat16 [4, 2, 128, 128], replicated, may hold values from -0.375 to 0.375
- beam_phase: float32 [4, 64], replicated, may hold values from -3.140625 to 3.140625
- tap_blocks: int32 [4, 2, 64], P(None, None, 'rng'), may hold values from 0 to 62, as said below
Outputs:
- image: bfloat16 [2, 512, 8192], P(None, 'pulse', 'rng')
The draws below stay inside these ranges and needn't reach their ends.
Inputs may be any that keep to these rules, and one draw needn't show every extreme that they name: tap_blocks[s, h, b] lies in the same aligned run of 32 range blocks as b and is never the last block of that run.
All inputs are finite; a program needn't handle non-finite values.
Results may differ from the reference program's by a relative error of at most 0.028.
Values may be sent and summed in bfloat16 or wider, within the bound.
A program may use at most 64 MiB of HBM per device.

```python
import jax
import jax.numpy as jnp
from jax import lax

BINS = 8192
TAPS = 128
AZ_HALF = 4
P_DEV = 32
BEAMS_DEV = 32
AZ_TAPS = 9
PULSES = 512
BEAMS = 512
BLOCKS = 64
BLOCKS_DEV = 32
SECTIONS = 4
N_PULSE = 16


def draw_tap_blocks(key, part):
    blocks = jnp.arange(BLOCKS, dtype=jnp.int32)
    base = blocks // BLOCKS_DEV * BLOCKS_DEV
    offsets = jax.random.randint(key, (SECTIONS, 2, BLOCKS), 0, BLOCKS_DEV - 1, dtype=jnp.int32)
    return (base[None, None, :] + offsets).astype(jnp.int32)


def shard_levels(rng, dims, split, least, top_value):
    gain = 1.0
    for dim, shards_of in split:
        heights = jax.random.uniform(jax.random.fold_in(jax.random.fold_in(rng, 6), dim), (shards_of,), jnp.float32, least / len(split), top_value / len(split))
        gain = gain * jnp.repeat(jnp.exp(heights), dims[dim] // shards_of).reshape((-1,) + (1,) * (len(dims) - 1 - dim))
    return gain


def centred(rng, shape, scale, limit, shards=(), kind=jnp.bfloat16):
    entries = scale * jax.random.normal(rng, shape, jnp.float32)
    if shards:
        entries = entries * shard_levels(rng, shape, shards, -0.22, 0.18)
    return jnp.clip(entries, -limit, limit).astype(kind)


def setup_inputs(seed: int = 0) -> dict:
    streams_of = jax.random.split(jax.random.key(seed), 9)
    raw_pulses = centred(streams_of[0], (2, PULSES, BINS), 1.0, 6.0, ((1, 16), (2, 2)))
    azimuth_taps = centred(streams_of[1], (2, AZ_TAPS), (2 * AZ_TAPS) ** -0.5, 1.5, (), jnp.float32)
    range_taps = centred(streams_of[2], (2, TAPS), (2 * TAPS) ** -0.5, 0.375)
    steering = centred(streams_of[3], (2, BEAMS_DEV, P_DEV), (2 * P_DEV) ** -0.5, 0.75)
    angle_mats = centred(streams_of[4], (SECTIONS, 2, BEAMS_DEV, BEAMS_DEV), (2 * BEAMS_DEV) ** -0.5, 0.75)
    range_resampler_matrices = centred(streams_of[5], (SECTIONS, 2, TAPS, TAPS), (2 * TAPS) ** -0.5, 0.375)
    beam_phase = jnp.clip(jax.random.uniform(streams_of[6], (SECTIONS, 2 * BEAMS_DEV), jnp.float32, -3.140625, 3.140625), -3.140625, 3.140625)
    tap_blocks = draw_tap_blocks(jax.random.fold_in(streams_of[8], 71), 0)
    return dict(raw_pulses=raw_pulses, azimuth_taps=azimuth_taps, range_taps=range_taps, steering=steering, angle_mats=angle_mats, range_resampler_matrices=range_resampler_matrices, beam_phase=beam_phase, tap_blocks=tap_blocks)


def azimuth(padded, azimuth_taps, count):
    real_sum = jnp.zeros((count, padded.shape[2]), jnp.float32)
    imag_sum = jnp.zeros((count, padded.shape[2]), jnp.float32)
    for offset in range(azimuth_taps.shape[1]):
        window = lax.slice_in_dim(padded, offset, offset + count, axis=1).astype(jnp.float32)
        real_sum = real_sum + azimuth_taps[0, offset] * window[0] - azimuth_taps[1, offset] * window[1]
        imag_sum = imag_sum + azimuth_taps[0, offset] * window[1] + azimuth_taps[1, offset] * window[0]
    return jnp.stack([real_sum, imag_sum]).astype(jnp.bfloat16)


def complex_form(matrix):
    first = jnp.stack([matrix[0], matrix[1]], axis=1)
    second = jnp.stack([-matrix[1], matrix[0]], axis=1)
    return jnp.stack([first, second])


def toeplitz_pair(range_taps):
    width = range_taps.shape[1]
    rows = jnp.arange(width, dtype=jnp.int32)[:, None]
    cols = jnp.arange(width, dtype=jnp.int32)[None, :]
    spacing = cols - rows
    nothing = jnp.zeros((), range_taps.dtype)
    current = jnp.where(spacing >= 0, jnp.take(range_taps, jnp.where(spacing >= 0, spacing, 0), axis=1), nothing)
    earlier = jnp.where(spacing < 0, jnp.take(range_taps, jnp.where(spacing < 0, spacing + width, 0), axis=1), nothing)
    return jnp.stack([complex_form(current), complex_form(earlier)])


def resample(subimage, angle_set, range_pair, phase_ramp_row, tap_rows, sector, sign):
    beams = subimage.shape[1]
    width = range_pair.shape[1]
    matrix = lax.dynamic_index_in_dim(angle_set, sector, 0, keepdims=False)
    turned = jnp.einsum("ab,cbr->car", matrix.astype(jnp.float32), subimage.astype(jnp.float32)).astype(jnp.bfloat16)
    blocked = turned.reshape(2, beams, -1, width)
    chosen = lax.dynamic_index_in_dim(tap_rows, sector, 0, keepdims=False).astype(jnp.int32)
    lower = jnp.take(blocked, chosen, axis=2)
    upper = jnp.take(blocked, chosen + 1, axis=2)
    moved = jnp.einsum("kcani,kij->canj", jnp.stack([lower, upper]).astype(jnp.float32), range_pair.astype(jnp.float32))
    moved = moved.reshape(2, beams, -1)
    angle = sign * lax.dynamic_slice_in_dim(phase_ramp_row, sector * beams, beams)[:, None]
    cosine = jnp.cos(angle)
    sine = jnp.sin(angle)
    return jnp.stack([moved[0] * cosine - moved[1] * sine, moved[0] * sine + moved[1] * cosine])


def reference(raw_pulses, azimuth_taps, range_taps, steering, angle_mats, range_resampler_matrices, beam_phase, tap_blocks):
    padded = jnp.pad(raw_pulses, ((0, 0), (AZ_HALF, AZ_HALF), (0, 0)))
    filtered = azimuth(padded, azimuth_taps, PULSES)
    blocked = filtered.reshape(2, PULSES, BLOCKS, TAPS)
    earlier = jnp.concatenate([jnp.zeros_like(blocked[:, :, :1]), blocked[:, :, :-1]], axis=2)
    weights = toeplitz_pair(range_taps)
    pulse_compressed_data = jnp.einsum("bcpni,bcioj->opnj", jnp.stack([blocked, earlier]).astype(jnp.float32), weights.astype(jnp.float32))
    pulse_compressed_data = pulse_compressed_data.astype(jnp.bfloat16).reshape(2, N_PULSE, P_DEV, BINS).astype(jnp.float32)
    steering_real = steering[0].astype(jnp.float32)
    steering_imaginary = steering[1].astype(jnp.float32)
    real_component = jnp.einsum("lx,nxd->nld", steering_real, pulse_compressed_data[0]) - jnp.einsum("lx,nxd->nld", steering_imaginary, pulse_compressed_data[1])
    imaginary_component = jnp.einsum("lx,nxd->nld", steering_real, pulse_compressed_data[1]) + jnp.einsum("lx,nxd->nld", steering_imaginary, pulse_compressed_data[0])
    subimages = jnp.stack([real_component, imaginary_component], axis=1).astype(jnp.bfloat16)
    for section in range(SECTIONS):
        def merged(member, subimages=subimages, section=section):
            parity = (member // (2 ** section)) % 2
            partner = member + (1 - 2 * parity) * (2 ** section)
            sign = (2 * parity - 1).astype(jnp.float32)
            self_contribution = resample(subimages[member], angle_mats[section], range_resampler_matrices[section], beam_phase[section], tap_blocks[section], parity, sign)
            other_term = resample(subimages[partner], angle_mats[section], range_resampler_matrices[section], beam_phase[section], tap_blocks[section], parity, -sign)
            return (self_contribution + other_term.astype(jnp.bfloat16).astype(jnp.float32)).astype(jnp.bfloat16)
        subimages = lax.map(merged, jnp.arange(N_PULSE, dtype=jnp.int32))
    return subimages.transpose(1, 0, 2, 3).reshape(2, BEAMS, BINS)
```

```python
import functools

import jax
import jax.numpy as jnp
from jax import lax
from jax.experimental import pallas as pl
from jax.experimental.pallas import tpu as pltpu
from jax.sharding import PartitionSpec as P

MESH = pl.DeviceIdType.MESH
F32 = jnp.float32
BF16 = jnp.bfloat16


def iota(shape, dim):
    return lax.broadcasted_iota(jnp.int32, shape, dim)


def mm(a, b):
    return jnp.dot(a, b, preferred_element_type=F32)


def placement(rows, cols, offset):
    return (iota((rows, cols), 1) == iota((rows, cols), 0) + offset).astype(BF16)


def azimuth_matrix(az, count, half):
    taps = 2 * half + 1
    shape = (2 * count, 2 * count + 4 * half)
    row, col = iota(shape, 0), iota(shape, 1)
    upper = row >= count
    pulse = jnp.where(upper, row - count, row)
    own = 2 * count
    low, high = own + 2 * half, own + 4 * half
    part = jnp.where(
        col < own,
        (col >= count).astype(jnp.int32),
        jnp.where(col < low, (col >= own + half).astype(jnp.int32), (col >= low + half).astype(jnp.int32)),
    )
    source = jnp.where(
        col < own,
        col - count * part,
        jnp.where(col < low, col - own - half * part - half, col - low - half * part + count),
    )
    lag = source - pulse + half
    same = upper == (part == 1)
    total = jnp.zeros(shape, F32)
    for k in range(taps):
        re, im = az[0, k], az[1, k]
        value = jnp.where(same, re, jnp.where(upper, im, -im))
        total = total + jnp.where(lag == k, value, 0.0)
    return total


def toeplitz(taps_row, width):
    rows = jnp.broadcast_to(taps_row, (width, width))
    return pltpu.roll(rows, 0, 1, stride=1, stride_axis=0)


def kernel(n, nr, raw, az, rt, st, am, rr, bp, tb, out,
           edge_out, edge_in, rim_out, rim_in, filt, x, turned, sendb, recvb, own, cs, w,
           edge_send, edge_recv, rim_send, rim_recv, send_sem, recv_sem):
    me, rn = lax.axis_index("pulse"), lax.axis_index("rng")
    count, bins = raw.shape[1], raw.shape[2]
    width = rt.shape[1]
    blocks = bins // width
    half = az.shape[1] // 2
    sections = n.bit_length() - 1
    chunks = sendb.shape[1]
    span = bins // chunks
    per = span // width

    def partner(s):
        mask = 2**s
        return me + mask - 2 * mask * ((me // mask) % 2)

    barrier = pltpu.get_barrier_semaphore()
    for s in range(sections):
        pl.semaphore_signal(barrier, inc=1, device_id=(partner(s), rn), device_id_type=MESH)
    for cond, target in ((me > 0, (me - 1, rn)), (me < n - 1, (me + 1, rn)),
                         (rn > 0, (me, rn - 1)), (rn < nr - 1, (me, rn + 1))):
        @pl.when(cond)
        def _(target=target):
            pl.semaphore_signal(barrier, inc=1, device_id=target, device_id_type=MESH)
    arrivals = (sections + (me > 0).astype(jnp.int32) + (me < n - 1).astype(jnp.int32)
                + (rn > 0).astype(jnp.int32) + (rn < nr - 1).astype(jnp.int32))

    shape = (4 * half, 2 * count)
    row, col = iota(shape, 0), iota(shape, 1)
    tail = row >= 2 * half
    local = jnp.where(tail, row - 2 * half, row)
    second = (local >= half).astype(jnp.int32)
    pick = local - half * second + jnp.where(tail, count - half, 0) + count * second
    chooser = (col == pick).astype(BF16)
    for c in range(chunks):
        cols = slice(c * span, (c + 1) * span)
        both = jnp.concatenate([raw[0, :, cols], raw[1, :, cols]], axis=0)
        edges = mm(chooser, both)
        edge_out[0, :, cols] = edges[: 2 * half].astype(BF16)
        edge_out[1, :, cols] = edges[2 * half :].astype(BF16)

    pl.semaphore_wait(barrier, arrivals)

    to_low = pltpu.make_async_remote_copy(
        edge_out.at[0], edge_in.at[1], edge_send.at[0], edge_recv.at[1],
        device_id=(me - 1, rn), device_id_type=MESH)
    to_high = pltpu.make_async_remote_copy(
        edge_out.at[1], edge_in.at[0], edge_send.at[1], edge_recv.at[0],
        device_id=(me + 1, rn), device_id_type=MESH)

    @pl.when(me > 0)
    def _():
        to_low.start()

    @pl.when(me < n - 1)
    def _():
        to_high.start()

    p0, p1 = placement(count, 2 * count, 0), placement(count, 2 * count, count)
    s_re, s_im = st[0], st[1]
    steer = jnp.concatenate([mm(s_re, p0) - mm(s_im, p1), mm(s_im, p0) + mm(s_re, p1)], axis=0)
    mix = jnp.dot(steer, azimuth_matrix(az, count, half), precision=lax.Precision.HIGHEST,
                  preferred_element_type=F32)
    first = mix.astype(BF16)
    rest = mix - first.astype(F32)
    second_part = rest.astype(BF16)
    third_part = (rest - second_part.astype(F32)).astype(BF16)
    taps = rt[...].astype(F32)
    rows, cols_ = iota((width, width), 0), iota((width, width), 1)
    full = [toeplitz(taps[c : c + 1], width) for c in range(2)]
    for e, keep in enumerate((cols_ >= rows, cols_ < rows)):
        m0, m1 = (jnp.where(keep, f, 0.0) for f in full)
        w[(2 * e) * width : (2 * e + 1) * width, :width] = m0.astype(BF16)
        w[(2 * e) * width : (2 * e + 1) * width, width:] = m1.astype(BF16)
        w[(2 * e + 1) * width : (2 * e + 2) * width, :width] = (-m1).astype(BF16)
        w[(2 * e + 1) * width : (2 * e + 2) * width, width:] = m0.astype(BF16)
    beams = am.shape[2]
    for s in range(sections):
        parity = (me // 2**s) % 2
        sign = (2 * parity - 1).astype(F32)
        for i, sector in enumerate((1 - parity, parity)):
            phases = jnp.broadcast_to(bp[s : s + 1, :], (beams, 2 * beams))
            hit = iota((beams, 2 * beams), 1) == iota((beams, 2 * beams), 0) + sector * beams
            angle = sign * jnp.sum(jnp.where(hit, phases, 0.0), axis=1, keepdims=True)
            angle = jnp.broadcast_to(angle, (beams, width))
            cs[s, i, 0] = jnp.cos(angle)
            cs[s, i, 1] = jnp.sin(angle)

    @pl.when(me == 0)
    def _():
        edge_in[0] = jnp.zeros(edge_in.shape[1:], BF16)

    @pl.when(me == n - 1)
    def _():
        edge_in[1] = jnp.zeros(edge_in.shape[1:], BF16)

    @pl.when(me > 0)
    def _():
        to_high.wait_recv()

    @pl.when(me < n - 1)
    def _():
        to_low.wait_recv()

    to_right = pltpu.make_async_remote_copy(
        rim_out, rim_in, rim_send, rim_recv, device_id=(me, rn + 1), device_id_type=MESH)
    for c in reversed(range(chunks)):
        cols = slice(c * span, (c + 1) * span)
        gathered = jnp.concatenate([raw[0, :, cols], raw[1, :, cols], edge_in[0, :, cols], edge_in[1, :, cols]], axis=0)
        value = (mm(first, gathered) + mm(second_part, gathered) + mm(third_part, gathered)).astype(BF16)
        for j in range(per):
            b = c * per + j + 1
            for part in range(2):
                filt[part, b * count : (b + 1) * count, :] = value[
                    part * count : (part + 1) * count, j * width : (j + 1) * width]
        if c == chunks - 1:
            for part in range(2):
                rim_out[part] = value[part * count : (part + 1) * count, span - width :]

            @pl.when(rn < nr - 1)
            def _():
                to_right.start()

    @pl.when(rn == 0)
    def _():
        filt[:, :count, :] = jnp.zeros((2, count, width), BF16)

    @pl.when(rn > 0)
    def _():
        to_right.wait_recv()
        filt[:, :count, :] = rim_in[...]

    weights = w[...]
    for c in range(chunks):
        r0 = c * per * count
        r1 = r0 + per * count
        lhs = jnp.concatenate(
            [filt[0, r0 + count : r1 + count, :], filt[1, r0 + count : r1 + count, :],
             filt[0, r0:r1, :], filt[1, r0:r1, :]], axis=1)
        res = mm(lhs, weights).astype(BF16)
        for j in range(per):
            b = c * per + j
            for part in range(2):
                x[part * count : (part + 1) * count, b * width : (b + 1) * width] = res[
                    j * count : (j + 1) * count, part * width : (part + 1) * width]

    start = rn * blocks
    for s in range(sections):
        parity = (me // 2**s) % 2
        sectors = (1 - parity, parity)
        a_out, a_own = am[s, 1 - parity], am[s, parity]
        a2 = jnp.concatenate([mm(a_out, p0), mm(a_out, p1), mm(a_own, p0), mm(a_own, p1)], axis=0).astype(BF16)
        for c in range(chunks):
            value = mm(a2, x[:, c * span : (c + 1) * span]).astype(BF16)
            for j in range(per):
                for i in range(2):
                    turned[i, c * per + j] = value[
                        i * 2 * beams : (i + 1) * 2 * beams, j * width : (j + 1) * width]
        pair = jnp.concatenate([rr[s, 0], rr[s, 1]], axis=0)

        def moved(i, c):
            lhs = []
            for j in range(per):
                t = jnp.maximum(tb[s, sectors[i], c * per + j] - start, 0)
                lhs.append(jnp.concatenate([turned[i, t], turned[i, t + 1]], axis=1))
            res = mm(jnp.concatenate(lhs, axis=0), pair)
            cosine, sine = cs[s, i, 0], cs[s, i, 1]
            for j in range(per):
                re = res[2 * j * beams : (2 * j + 1) * beams]
                im = res[(2 * j + 1) * beams : (2 * j + 2) * beams]
                yield j, re * cosine - im * sine, re * sine + im * cosine

        copies = []
        for c in range(chunks):
            for j, re, im in moved(0, c):
                sendb[s, c, :beams, j * width : (j + 1) * width] = re.astype(BF16)
                sendb[s, c, beams:, j * width : (j + 1) * width] = im.astype(BF16)
            copy = pltpu.make_async_remote_copy(
                sendb.at[s, c], recvb.at[s, c], send_sem.at[s, c], recv_sem.at[s, c],
                device_id=(partner(s), rn), device_id_type=MESH)
            copy.start()
            copies.append(copy)
        for c in range(chunks):
            for j, re, im in moved(1, c):
                b = c * per + j
                own[:beams, b * width : (b + 1) * width] = re
                own[beams:, b * width : (b + 1) * width] = im
        for c in range(chunks):
            copies[c].wait_recv()
            cols = slice(c * span, (c + 1) * span)
            merged = (own[:, cols] + recvb[s, c].astype(F32)).astype(BF16)
            if s == sections - 1:
                out[0, :, cols] = merged[:beams]
                out[1, :, cols] = merged[beams:]
            else:
                x[:, cols] = merged
        for copy in copies:
            copy.wait_send()

    @pl.when(me > 0)
    def _():
        to_low.wait_send()

    @pl.when(me < n - 1)
    def _():
        to_high.wait_send()

    @pl.when(rn < nr - 1)
    def _():
        to_right.wait_send()


def solution(mesh):
    n, nr = mesh.shape["pulse"], mesh.shape["rng"]

    def local(raw_pulses, azimuth_taps, range_taps, steering, angle_mats,
              range_resampler_matrices, beam_phase, tap_blocks):
        count, bins = raw_pulses.shape[1:]
        width = range_taps.shape[1]
        half = azimuth_taps.shape[1] // 2
        blocks = bins // width
        sections = n.bit_length() - 1
        chunks = 4
        rows = 2 * count
        vmem = pl.BlockSpec(memory_space=pltpu.VMEM)
        smem = pl.BlockSpec(memory_space=pltpu.SMEM)
        dma = pltpu.SemaphoreType.DMA
        return pl.pallas_call(
            functools.partial(kernel, n, nr),
            out_shape=jax.ShapeDtypeStruct((2, count, bins), BF16),
            in_specs=[vmem, smem, vmem, vmem, vmem, vmem, vmem, smem],
            out_specs=vmem,
            scratch_shapes=[
                pltpu.VMEM((2, 2 * half, bins), BF16),
                pltpu.VMEM((2, 2 * half, bins), BF16),
                pltpu.VMEM((2, count, width), BF16),
                pltpu.VMEM((2, count, width), BF16),
                pltpu.VMEM((2, (blocks + 1) * count, width), BF16),
                pltpu.VMEM((rows, bins), BF16),
                pltpu.VMEM((2, blocks, rows, width), BF16),
                pltpu.VMEM((sections, chunks, rows, bins // chunks), BF16),
                pltpu.VMEM((sections, chunks, rows, bins // chunks), BF16),
                pltpu.VMEM((rows, bins), F32),
                pltpu.VMEM((sections, 2, 2, count, width), F32),
                pltpu.VMEM((4 * width, 2 * width), BF16),
                dma((2,)), dma((2,)), dma, dma,
                dma((sections, chunks)), dma((sections, chunks)),
            ],
            compiler_params=pltpu.CompilerParams(collective_id=0, has_side_effects=True),
        )(raw_pulses, azimuth_taps, range_taps, steering, angle_mats,
          range_resampler_matrices, beam_phase, tap_blocks)

    return jax.shard_map(
        local,
        mesh=mesh,
        in_specs=(P(None, "pulse", "rng"), P(), P(), P(), P(), P(), P(), P(None, None, "rng")),
        out_specs=P(None, "pulse", "rng"),
        check_vma=False,
    )
```

```python
import functools

import jax
import jax.numpy as jnp
from jax import lax
from jax.experimental import pallas as pl
from jax.experimental.pallas import tpu as pltpu
from jax.sharding import PartitionSpec as P

MESH = pl.DeviceIdType.MESH
F32 = jnp.float32
BF16 = jnp.bfloat16


def iota(shape, dim):
    return lax.broadcasted_iota(jnp.int32, shape, dim)


def mm(a, b):
    return jnp.dot(a, b, preferred_element_type=F32)


def placement(rows, cols, offset):
    return (iota((rows, cols), 1) == iota((rows, cols), 0) + offset).astype(BF16)


def azimuth_matrix(az, count, half):
    taps = 2 * half + 1
    shape = (2 * count, 2 * count + 4 * half)
    row, col = iota(shape, 0), iota(shape, 1)
    upper = row >= count
    pulse = jnp.where(upper, row - count, row)
    own = 2 * count
    low, high = own + 2 * half, own + 4 * half
    part = jnp.where(
        col < own,
        (col >= count).astype(jnp.int32),
        jnp.where(col < low, (col >= own + half).astype(jnp.int32), (col >= low + half).astype(jnp.int32)),
    )
    source = jnp.where(
        col < own,
        col - count * part,
        jnp.where(col < low, col - own - half * part - half, col - low - half * part + count),
    )
    lag = source - pulse + half
    same = upper == (part == 1)
    total = jnp.zeros(shape, F32)
    for k in range(taps):
        re, im = az[0, k], az[1, k]
        value = jnp.where(same, re, jnp.where(upper, im, -im))
        total = total + jnp.where(lag == k, value, 0.0)
    return total


def toeplitz(taps_row, width):
    rows = jnp.broadcast_to(taps_row, (width, width))
    return pltpu.roll(rows, 0, 1, stride=1, stride_axis=0)


def kernel(n, nr, raw, az, rt, st, am, rr, bp, tb, out,
           edge_out, edge_in, rim_out, rim_in, filt, held, far, near, turned, late, message, own, duals, singles, w,
           edge_send, edge_recv, rim_send, rim_recv, send_sem, recv_sem):
    me, rn = lax.axis_index("pulse"), lax.axis_index("rng")
    count, bins = raw.shape[1], raw.shape[2]
    width = rt.shape[1]
    blocks = bins // width
    half = az.shape[1] // 2
    sections = n.bit_length() - 1
    chunks = held.shape[1]
    plain = sections - 3
    span = bins // chunks
    per = span // width

    def partner(s):
        mask = 2**s
        return me + mask - 2 * mask * ((me // mask) % 2)

    barrier = pltpu.get_barrier_semaphore()
    for s in range(sections):
        pl.semaphore_signal(barrier, inc=1, device_id=(partner(s), rn), device_id_type=MESH)
    for cond, target in ((me > 0, (me - 1, rn)), (me < n - 1, (me + 1, rn)),
                         (rn > 0, (me, rn - 1)), (rn < nr - 1, (me, rn + 1))):
        @pl.when(cond)
        def _(target=target):
            pl.semaphore_signal(barrier, inc=1, device_id=target, device_id_type=MESH)
    arrivals = (sections + (me > 0).astype(jnp.int32) + (me < n - 1).astype(jnp.int32)
                + (rn > 0).astype(jnp.int32) + (rn < nr - 1).astype(jnp.int32))

    shape = (4 * half, 2 * count)
    row, col = iota(shape, 0), iota(shape, 1)
    tail = row >= 2 * half
    local = jnp.where(tail, row - 2 * half, row)
    second = (local >= half).astype(jnp.int32)
    pick = local - half * second + jnp.where(tail, count - half, 0) + count * second
    chooser = (col == pick).astype(BF16)
    for c in range(chunks):
        cols = slice(c * span, (c + 1) * span)
        both = jnp.concatenate([raw[0, :, cols], raw[1, :, cols]], axis=0)
        edges = mm(chooser, both)
        edge_out[0, :, cols] = edges[: 2 * half].astype(BF16)
        edge_out[1, :, cols] = edges[2 * half :].astype(BF16)

    pl.semaphore_wait(barrier, arrivals)

    to_low = pltpu.make_async_remote_copy(
        edge_out.at[0], edge_in.at[1], edge_send.at[0], edge_recv.at[1],
        device_id=(me - 1, rn), device_id_type=MESH)
    to_high = pltpu.make_async_remote_copy(
        edge_out.at[1], edge_in.at[0], edge_send.at[1], edge_recv.at[0],
        device_id=(me + 1, rn), device_id_type=MESH)

    @pl.when(me > 0)
    def _():
        to_low.start()

    @pl.when(me < n - 1)
    def _():
        to_high.start()

    p0, p1 = placement(count, 2 * count, 0), placement(count, 2 * count, count)
    s_re, s_im = st[0], st[1]
    steer = jnp.concatenate([mm(s_re, p0) - mm(s_im, p1), mm(s_im, p0) + mm(s_re, p1)], axis=0)
    mix = jnp.dot(steer, azimuth_matrix(az, count, half), precision=lax.Precision.HIGHEST,
                  preferred_element_type=F32)
    first = mix.astype(BF16)
    rest = mix - first.astype(F32)
    second_part = rest.astype(BF16)
    third_part = (rest - second_part.astype(F32)).astype(BF16)
    taps = rt[...].astype(F32)
    rows, cols_ = iota((width, width), 0), iota((width, width), 1)
    full = [toeplitz(taps[c : c + 1], width) for c in range(2)]
    for e, keep in enumerate((cols_ >= rows, cols_ < rows)):
        m0, m1 = (jnp.where(keep, f, 0.0) for f in full)
        w[(2 * e) * width : (2 * e + 1) * width, :width] = m0.astype(BF16)
        w[(2 * e) * width : (2 * e + 1) * width, width:] = m1.astype(BF16)
        w[(2 * e + 1) * width : (2 * e + 2) * width, :width] = (-m1).astype(BF16)
        w[(2 * e + 1) * width : (2 * e + 2) * width, width:] = m0.astype(BF16)
    beams = am.shape[2]

    def parity(s):
        return (me // 2**s) % 2

    def turning(s, sector, terms):
        columns = 2 * 2 * beams * terms
        sign = (2 * parity(s) - 1).astype(F32)
        phases = jnp.broadcast_to(bp[s : s + 1, :], (beams, 2 * beams))
        hit = iota((beams, 2 * beams), 1) == iota((beams, 2 * beams), 0) + sector * beams
        angle = sign * jnp.sum(jnp.where(hit, phases, 0.0), axis=1, keepdims=True)
        angle = jnp.broadcast_to(angle, (beams, 128))
        cosine, sine = jnp.cos(angle)[:, :1], jnp.sin(angle)[:, :1]
        beam, column = iota((beams, columns), 0), iota((beams, columns), 1)
        real, imag, other = (jnp.zeros((beams, columns), jnp.bool_) for _ in range(3))
        for k in range(2 * terms):
            base = 2 * beams * k
            real = real | (column == beam + base)
            imag = imag | (column == beam + base + beams)
            if k % terms == 1:
                other = other | ((column >= base) & (column < base + 2 * beams))
        matrix = am[s, sector]
        on_real = mm(matrix, real.astype(BF16))
        on_imag = mm(matrix, imag.astype(BF16))
        turn = jnp.where(other, -sine, sine)
        whole = jnp.concatenate([cosine * on_real - turn * on_imag, turn * on_real + cosine * on_imag], axis=0)
        lead = whole.astype(BF16).astype(F32)
        return jnp.where(iota(whole.shape, 1) < columns // 2, lead, whole - lead).astype(BF16)

    for s in range(plain + 1):
        duals[s] = turning(s, parity(s), 2)
    singles[0] = turning(plain + 1, 1 - parity(plain + 1), 1)
    singles[1] = turning(plain + 1, parity(plain + 1), 1)
    duals[plain + 1] = turning(plain + 2, parity(plain + 2), 2)

    @pl.when(me == 0)
    def _():
        edge_in[0] = jnp.zeros(edge_in.shape[1:], BF16)

    @pl.when(me == n - 1)
    def _():
        edge_in[1] = jnp.zeros(edge_in.shape[1:], BF16)

    @pl.when(me > 0)
    def _():
        to_high.wait_recv()

    @pl.when(me < n - 1)
    def _():
        to_low.wait_recv()

    to_right = pltpu.make_async_remote_copy(
        rim_out, rim_in, rim_send, rim_recv, device_id=(me, rn + 1), device_id_type=MESH)
    for c in reversed(range(chunks)):
        cols = slice(c * span, (c + 1) * span)
        gathered = jnp.concatenate([raw[0, :, cols], raw[1, :, cols], edge_in[0, :, cols], edge_in[1, :, cols]], axis=0)
        value = (mm(first, gathered) + mm(second_part, gathered) + mm(third_part, gathered)).astype(BF16)
        for j in range(per):
            b = c * per + j + 1
            for part in range(2):
                filt[part, b * count : (b + 1) * count, :] = value[
                    part * count : (part + 1) * count, j * width : (j + 1) * width]
        if c == chunks - 1:
            for part in range(2):
                rim_out[part] = value[part * count : (part + 1) * count, span - width :]

            @pl.when(rn < nr - 1)
            def _():
                to_right.start()

    @pl.when(rn == 0)
    def _():
        filt[:, :count, :] = jnp.zeros((2, count, width), BF16)

    @pl.when(rn > 0)
    def _():
        to_right.wait_recv()
        filt[:, :count, :] = rim_in[...]

    copies = []

    def send(source, target, kind, c, s):
        copy = pltpu.make_async_remote_copy(
            source, target, send_sem.at[kind, c], recv_sem.at[kind, c],
            device_id=(partner(s), rn), device_id_type=MESH)
        copy.start()
        return copy

    def arrived(target, kind, c):
        pltpu.make_async_remote_copy(
            target, target, send_sem.at[kind, c], recv_sem.at[kind, c],
            device_id=(partner(0), rn), device_id_type=MESH).wait_recv()

    weights = w[...]
    for c in range(chunks):
        r0 = c * per * count
        r1 = r0 + per * count
        lhs = jnp.concatenate(
            [filt[0, r0 + count : r1 + count, :], filt[1, r0 + count : r1 + count, :],
             filt[0, r0:r1, :], filt[1, r0:r1, :]], axis=1)
        res = mm(lhs, weights).astype(BF16)
        for j in range(per):
            for part in range(2):
                held[0, c, part * count : (part + 1) * count, j * width : (j + 1) * width] = res[
                    j * count : (j + 1) * count, part * width : (part + 1) * width]
        if plain:
            copies.append(send(held.at[0, c], near.at[0, c], 0, c, 0))

    start = rn * blocks

    def turn(matrix, sources, c):
        parts = [source[c] for source in sources]
        value = mm(matrix, jnp.concatenate(parts + parts, axis=0)).astype(BF16)
        for j in range(per):
            turned[c * per + j] = value[:, j * width : (j + 1) * width]

    def move(s, sector, c):
        pair = jnp.concatenate([rr[s, 0], rr[s, 1]], axis=0)
        lhs = []
        for j in range(per):
            t = jnp.maximum(tb[s, sector, c * per + j] - start, 0)
            lhs.append(jnp.concatenate([turned[t], turned[t + 1]], axis=1))
        res = mm(jnp.concatenate(lhs, axis=0), pair)
        return jnp.concatenate([res[2 * j * beams : 2 * (j + 1) * beams] for j in range(per)], axis=1)

    def apply(matrix, sources, s, sector, target, then=None):
        for c in range(chunks):
            turn(matrix, sources, c)
        for c in range(chunks):
            target[c] = move(s, sector, c).astype(target.dtype)
            if then is not None:
                then(c)

    k, y, z, yz = plain, plain, plain + 1, plain + 2

    def pass_on(s, c):
        copies.append(send(held.at[s, c], near.at[s, c], s, c, s))

    def to_far(c):
        copies.append(send(held.at[k, c], far.at[0, c], z, c, k + 2))
        pass_on(k, c)

    for s in range(plain):
        for c in range(chunks):
            arrived(near.at[s, c], s, c)
        follow = to_far if s + 1 == plain else functools.partial(pass_on, s + 1)
        apply(duals[s], (held.at[s], near.at[s]), s, parity(s), held.at[s + 1], follow)
    if not plain:
        for c in range(chunks):
            to_far(c)

    def relay(c):
        arrived(far.at[0, c], z, c)
        copies.append(send(far.at[0, c], far.at[1, c], yz, c, k))

    early = chunks // 2
    for c in range(early):
        relay(c)
    for c in range(chunks):
        arrived(near.at[k, c], y, c)
    apply(duals[k], (held.at[k], near.at[k]), k, parity(k), late.at[0])
    for c in range(early, chunks):
        relay(c)
    out_half, own_half = 1 - parity(k + 1), parity(k + 1)
    apply(singles[0], (late.at[0],), k + 1, out_half, late.at[2])
    for c in range(chunks):
        arrived(far.at[1, c], yz, c)
    apply(duals[k], (far.at[0], far.at[1]), k, parity(k), late.at[1])
    apply(singles[0], (late.at[1],), k + 1, out_half, late.at[3])

    def deliver(c):
        copies.append(send(message.at[0, c], message.at[1, c], plain + 3, c, k + 1))

    apply(duals[k + 1], (late.at[2], late.at[3]), k + 2, parity(k + 2), message.at[0], deliver)
    apply(singles[1], (late.at[0],), k + 1, own_half, late.at[2])
    apply(singles[1], (late.at[1],), k + 1, own_half, late.at[3])
    apply(duals[k + 1], (late.at[2], late.at[3]), k + 2, parity(k + 2), own)
    for c in range(chunks):
        arrived(message.at[1, c], plain + 3, c)
        merged = (own[c] + message[1, c].astype(F32)).astype(BF16)
        cols = slice(c * span, (c + 1) * span)
        out[0, :, cols] = merged[:beams]
        out[1, :, cols] = merged[beams:]
    for copy in copies:
        copy.wait_send()

    @pl.when(me > 0)
    def _():
        to_low.wait_send()

    @pl.when(me < n - 1)
    def _():
        to_high.wait_send()

    @pl.when(rn < nr - 1)
    def _():
        to_right.wait_send()


def solution(mesh):
    n, nr = mesh.shape["pulse"], mesh.shape["rng"]

    def local(raw_pulses, azimuth_taps, range_taps, steering, angle_mats,
              range_resampler_matrices, beam_phase, tap_blocks):
        count, bins = raw_pulses.shape[1:]
        width = range_taps.shape[1]
        half = azimuth_taps.shape[1] // 2
        blocks = bins // width
        sections = n.bit_length() - 1
        chunks = 8
        plain = sections - 3
        rows = 2 * count
        image = (chunks, rows, bins // chunks)
        vmem = pl.BlockSpec(memory_space=pltpu.VMEM)
        smem = pl.BlockSpec(memory_space=pltpu.SMEM)
        dma = pltpu.SemaphoreType.DMA
        return pl.pallas_call(
            functools.partial(kernel, n, nr),
            out_shape=jax.ShapeDtypeStruct((2, count, bins), BF16),
            in_specs=[vmem, smem, vmem, vmem, vmem, vmem, vmem, smem],
            out_specs=vmem,
            scratch_shapes=[
                pltpu.VMEM((2, 2 * half, bins), BF16),
                pltpu.VMEM((2, 2 * half, bins), BF16),
                pltpu.VMEM((2, count, width), BF16),
                pltpu.VMEM((2, count, width), BF16),
                pltpu.VMEM((2, (blocks + 1) * count, width), BF16),
                pltpu.VMEM((plain + 1, *image), BF16),
                pltpu.VMEM((2, *image), BF16),
                pltpu.VMEM((plain + 1, *image), BF16),
                pltpu.VMEM((blocks, rows, width), BF16),
                pltpu.VMEM((4, *image), BF16),
                pltpu.VMEM((2, *image), BF16),
                pltpu.VMEM(image, F32),
                pltpu.VMEM((plain + 2, rows, 4 * rows), BF16),
                pltpu.VMEM((2, rows, 2 * rows), BF16),
                pltpu.VMEM((4 * width, 2 * width), BF16),
                dma((2,)), dma((2,)), dma, dma,
                dma((plain + 4, chunks)), dma((plain + 4, chunks)),
            ],
            compiler_params=pltpu.CompilerParams(collective_id=0, has_side_effects=True),
        )(raw_pulses, azimuth_taps, range_taps, steering, angle_mats,
          range_resampler_matrices, beam_phase, tap_blocks)

    return jax.shard_map(
        local,
        mesh=mesh,
        in_specs=(P(None, "pulse", "rng"), P(), P(), P(), P(), P(), P(), P(None, None, "rng")),
        out_specs=P(None, "pulse", "rng"),
        check_vma=False,
    )
```
